32 devices in a mesh: tm: 4 (over x, core), space: 8 (over z, y).
Axes of the slice: x: 2, y: 2, z: 4, core: 2. Of those that a mesh axis runs over, the one named last changes fastest.
Arguments:
- state_rhs: float32 [32, 16, 128, 128], P('tm', 'space'), may hold values from -5 to 9
- adjoint_rhs: float32 [32, 16, 128, 128], P('tm', 'space'), may hold values from -5 to 9
- reaction: float32 [16, 128, 128], P('space'), may hold values from 0.01 to 1
Outputs:
- state_out: float32 [32, 16, 128, 128], P('tm', 'space')
- adjoint_out: float32 [32, 16, 128, 128], P('tm', 'space')
The draws below stay inside these ranges and needn't reach their ends.
All inputs are finite; a program needn't handle non-finite values.
Results may differ from the reference program's by a relative error of at most 0.00021.
Values sent between devices are 32-bit elements; how exact they have to be, the bound alone decides.
A program may use at most 64 MiB of HBM per device.

```python
import math
import jax
import jax.numpy as jnp
from jax import lax

STEPS = 32
SWEEPS = 12
NX = 128
NY = 128
NZ = 16


def smooth_source(key, salt):
    folded = jax.random.fold_in(key, salt)
    phase_key, noise_key = jax.random.split(folded, 2)
    phases = jax.random.uniform(phase_key, (4,), jnp.float32, 0.0, 2.0 * math.pi)
    moments = jnp.arange(STEPS, dtype=jnp.float32)
    depths = jnp.arange(NZ, dtype=jnp.float32)
    across = jnp.arange(NX, dtype=jnp.float32)
    along = jnp.arange(NY, dtype=jnp.float32)
    amplitude = 1.5
    contrast = 0.4
    noise = jnp.clip(jax.random.normal(noise_key, (STEPS, NZ, NX, NY), jnp.float32), -5.0, 5.0)
    profile = 1.0 + 0.3 * jnp.cos(2.0 * math.pi * moments / STEPS + phases[0])
    strength = jnp.exp(contrast * jnp.cos(2.0 * math.pi * depths / 16.0 + phases[1]))
    lateral = 1.0 + 0.3 * jnp.cos(2.0 * math.pi * across / NX + phases[2])[:, None] * jnp.cos(2.0 * math.pi * along / NY + phases[3])[None, :]
    smooth = amplitude * profile[:, None, None, None] * strength[None, :, None, None] * lateral[None, None, :, :]
    return smooth + noise


def draw_state_rhs(key, part):
    return smooth_source(key, 11)


def draw_adjoint_rhs(key, part):
    return smooth_source(key, 23)


def draw_reaction(key, part):
    spread = jax.random.uniform(jax.random.fold_in(key, 37), (NZ, NX, NY), jnp.float32, 0.0, 1.0)
    return 0.01 * jnp.exp(math.log(100.0) * spread)


def setup_inputs(seed: int = 0) -> dict:
    arg_keys = jax.random.split(jax.random.key(seed), 4)
    return {
        "state_rhs": draw_state_rhs(jax.random.fold_in(arg_keys[3], 71), 0),
        "adjoint_rhs": draw_adjoint_rhs(jax.random.fold_in(arg_keys[3], 71), 0),
        "reaction": draw_reaction(jax.random.fold_in(arg_keys[3], 71), 0),
    }


ALPHA = 0.1
MU = 1.0
BETA = 1.0


def coefficients(reaction, freqs):
    turn = 2.0 * math.pi * freqs.astype(jnp.float32) / STEPS
    rate = math.exp(math.log(ALPHA) / STEPS)
    lam_re = 1.0 - rate * jnp.cos(turn)
    lam_im = rate * jnp.sin(turn)
    shaped = (-1,) + (1,) * reaction.ndim
    d_re = lam_re.reshape(shaped) + MU * (6.0 + reaction)
    d_im = jnp.broadcast_to(lam_im.reshape(shaped), d_re.shape)
    den_re = d_re * d_re - d_im * d_im + BETA * BETA
    den_im = 2.0 * d_re * d_im
    magnitude = den_re * den_re + den_im * den_im
    inv_re = den_re / magnitude
    inv_im = -den_im / magnitude
    return (d_re * inv_re - d_im * inv_im, d_re * inv_im + d_im * inv_re, BETA * inv_re, BETA * inv_im)


def block_solve(coefficient, source):
    q_re, q_im, r_re, r_im = coefficient
    y_real = source[..., 0, :, :, :]
    y_imag = source[..., 1, :, :, :]
    p_real = source[..., 2, :, :, :]
    p_imag = source[..., 3, :, :, :]
    new_yre = q_re * y_real - q_im * y_imag + (r_re * p_real - r_im * p_imag)
    new_yim = q_re * y_imag + q_im * y_real + (r_re * p_imag + r_im * p_real)
    new_pre = q_re * p_real - q_im * p_imag - (r_re * y_real - r_im * y_imag)
    new_pim = q_re * p_imag + q_im * p_real - (r_re * y_imag + r_im * y_real)
    return jnp.stack((new_yre, new_yim, new_pre, new_pim), axis=-4)


def neighbour_sum(field):
    padded = jnp.pad(field, ((0, 0), (1, 1), (1, 1), (1, 1)))
    total = padded[:, 2:, 1:-1, 1:-1] + padded[:, :-2, 1:-1, 1:-1]
    total = total + padded[:, 1:-1, 2:, 1:-1] + padded[:, 1:-1, :-2, 1:-1]
    return total + padded[:, 1:-1, 1:-1, 2:] + padded[:, 1:-1, 1:-1, :-2]


def reference(state_rhs, adjoint_rhs, reaction):
    times = jnp.arange(STEPS, dtype=jnp.float32)
    growth = jnp.exp(math.log(ALPHA) * times / STEPS)[:, None, None, None]
    shrink = jnp.exp(-math.log(ALPHA) * times / STEPS)[:, None, None, None]
    state_hat = jnp.fft.fft(state_rhs * growth, axis=0)
    adjoint_hat = jnp.fft.fft(adjoint_rhs[::-1] * growth, axis=0)
    sources = jnp.stack((state_hat.real, state_hat.imag, adjoint_hat.real, adjoint_hat.imag), axis=1)

    def solve_one(inputs):
        freq_rhs, freq_index = inputs
        coefficient = tuple(member[0] for member in coefficients(reaction, freq_index[None]))
        field = block_solve(coefficient, freq_rhs)

        def sweep(sweep_index, current):
            return block_solve(coefficient, freq_rhs + MU * neighbour_sum(current))

        return lax.fori_loop(0, SWEEPS - 1, sweep, field)

    solved = lax.map(solve_one, (sources, jnp.arange(STEPS, dtype=jnp.int32)))
    state_back = jnp.fft.ifft(solved[:, 0] + 1j * solved[:, 1], axis=0).real * shrink
    adjoint_back = (jnp.fft.ifft(solved[:, 2] + 1j * solved[:, 3], axis=0).real * shrink)[::-1]
    return state_back, adjoint_back
```

```python
import functools
import math

import jax
import jax.numpy as jnp
import numpy as np
from jax import lax
from jax.experimental import pallas as pl
from jax.experimental.pallas import tpu as pltpu
from jax.sharding import PartitionSpec as P

STEPS = 32
SWEEPS = 12


ALPHA = 0.1
MU = 1.0
BETA = 1.0


def padded_2(cells, sides, width):
    for axis, dim in sides:
        count = lax.axis_size(axis)
        ends = count - 1
        head = lax.slice_in_dim(cells, 0, width, axis=dim)
        tail = lax.slice_in_dim(cells, cells.shape[dim] - width, cells.shape[dim], axis=dim)
        cells = jnp.concatenate(
            [
                lax.ppermute(tail, axis, [(i, (i + 1) % count) for i in range(ends)]),
                cells,
                lax.ppermute(head, axis, [((i + 1) % count, i) for i in range(ends)]),
            ],
            axis=dim,
        )
    return cells


def coefficients(reaction, freqs):
    turn = 2.0 * math.pi * freqs.astype(jnp.float32) / STEPS
    rate = math.exp(math.log(ALPHA) / STEPS)
    lam_re = 1.0 - rate * jnp.cos(turn)
    lam_im = rate * jnp.sin(turn)
    shaped = (-1,) + (1,) * reaction.ndim
    d_re = lam_re.reshape(shaped) + MU * (6.0 + reaction)
    d_im = jnp.broadcast_to(lam_im.reshape(shaped), d_re.shape)
    den_re = d_re * d_re - d_im * d_im + BETA * BETA
    den_im = 2.0 * d_re * d_im
    magnitude = den_re * den_re + den_im * den_im
    inv_re = den_re / magnitude
    inv_im = -den_im / magnitude
    return (
        d_re * inv_re - d_im * inv_im,
        d_re * inv_im + d_im * inv_re,
        BETA * inv_re,
        BETA * inv_im,
    )


def block_solve(coefficient, source):
    q_re, q_im, r_re, r_im = coefficient
    y_real = source[..., 0, :, :, :]
    y_imag = source[..., 1, :, :, :]
    p_real = source[..., 2, :, :, :]
    p_imag = source[..., 3, :, :, :]
    new_yre = q_re * y_real - q_im * y_imag + (r_re * p_real - r_im * p_imag)
    new_yim = q_re * y_imag + q_im * y_real + (r_re * p_imag + r_im * p_real)
    new_pre = q_re * p_real - q_im * p_imag - (r_re * y_real - r_im * y_imag)
    new_pim = q_re * p_imag + q_im * p_real - (r_re * y_imag + r_im * y_real)
    return jnp.stack((new_yre, new_yim, new_pre, new_pim), axis=-4)


def neighbour_sum(zpadded):
    inner = zpadded[:, :, 1:-1]
    padded = jnp.pad(inner, ((0, 0), (0, 0), (0, 0), (1, 1), (1, 1)))
    total = zpadded[:, :, 2:] + zpadded[:, :, :-2]
    total = total + padded[:, :, :, 2:, 1:-1] + padded[:, :, :, :-2, 1:-1]
    return total + padded[:, :, :, 1:-1, 2:] + padded[:, :, :, 1:-1, :-2]


def effective(times, reverse):
    if reverse:
        return STEPS - 1 - times
    return times


def forward_table(freqs, times, reverse):
    moment = effective(times, reverse)
    phase = freqs[:, None] * moment[None, :] % STEPS
    angle = 2.0 * math.pi / STEPS * phase.astype(jnp.float32)
    growth = jnp.exp(math.log(ALPHA) * moment.astype(jnp.float32) / STEPS)[None, :]
    table = jnp.stack((jnp.cos(angle) * growth, -jnp.sin(angle) * growth), axis=1)
    return table.reshape(-1, times.shape[0])


def inverse_table(freqs, times, reverse):
    moment = effective(times, reverse)
    phase = moment[:, None] * freqs[None, :] % STEPS
    angle = 2.0 * math.pi / STEPS * phase.astype(jnp.float32)
    shrink = jnp.exp(-math.log(ALPHA) * moment.astype(jnp.float32) / STEPS)[:, None] / STEPS
    table = jnp.stack((jnp.cos(angle) * shrink, -jnp.sin(angle) * shrink), axis=2)
    return table.reshape(times.shape[0], -1)


def forward_pair(state_part, adjoint_part, freqs, times):
    rows = state_part.shape[0]
    state_hat = jnp.dot(
        forward_table(freqs, times, False),
        state_part.reshape(rows, -1),
        precision=lax.Precision.HIGHEST,
    )
    adjoint_hat = jnp.dot(
        forward_table(freqs, times, True),
        adjoint_part.reshape(rows, -1),
        precision=lax.Precision.HIGHEST,
    )
    return (state_hat, adjoint_hat)


def backward_pair(solved, freqs, times):
    count = solved.shape[0]
    slab = solved.shape[2:]
    flat_state = solved[:, 0:2].reshape(2 * count, -1)
    flat_adjoint = solved[:, 2:4].reshape(2 * count, -1)
    state_time = jnp.dot(
        inverse_table(freqs, times, False), flat_state, precision=lax.Precision.HIGHEST
    )
    adjoint_time = jnp.dot(
        inverse_table(freqs, times, True), flat_adjoint, precision=lax.Precision.HIGHEST
    )
    shaped = (times.shape[0],) + slab
    return (state_time.reshape(shaped), adjoint_time.reshape(shaped))


def body(state_rhs, adjoint_rhs, reaction):
    groups = lax.axis_size("tm")
    local_steps = state_rhs.shape[0]
    freq_count = STEPS // groups
    slab_shape = state_rhs.shape[1:]
    freqs = lax.axis_index("tm") * freq_count + jnp.arange(freq_count, dtype=jnp.int32)
    pieces = (
        lax.all_gather(state_rhs, "tm", axis=0, tiled=True),
        lax.all_gather(adjoint_rhs, "tm", axis=0, tiled=True),
    )
    rows = pieces[0].shape[0]
    times = jnp.arange(rows, dtype=jnp.int32)
    state_hat, adjoint_hat = forward_pair(pieces[0], pieces[1], freqs, times)
    state_hat, adjoint_hat = (state_hat, adjoint_hat)
    sources = jnp.concatenate(
        (
            state_hat.reshape((freq_count, 2) + slab_shape),
            adjoint_hat.reshape((freq_count, 2) + slab_shape),
        ),
        axis=1,
    )
    coefficient = coefficients(reaction, freqs)
    field = block_solve(coefficient, sources)

    def sweep(sweep_index, current):
        zpadded = padded_2(current, (("space", 2),), 1)
        return block_solve(coefficient, sources + MU * neighbour_sum(zpadded))

    solved = lax.fori_loop(0, SWEEPS - 1, sweep, field)
    times = jnp.arange(local_steps * lax.axis_size("tm"), dtype=jnp.int32)
    state_time, adjoint_time = backward_pair(solved, freqs, times)
    combined = lax.psum_scatter(
        jnp.stack((state_time, adjoint_time), axis=1), "tm", scatter_dimension=0, tiled=True
    )
    state_out = combined[:, 0]
    adjoint_out = combined[:, 1]
    return (state_out, adjoint_out)


MESH = pl.DeviceIdType.MESH


def cmul_const(factor, value):
    re, im = value
    a, b = float(factor.real), float(factor.imag)
    if abs(b) < 1e-12 and abs(a - 1.0) < 1e-12:
        return value
    if abs(a) < 1e-12:
        return (-im, re) if b > 0 else (im, -re)
    if abs(abs(a) - abs(b)) < 1e-12:
        sa, sb = math.copysign(1.0, a), math.copysign(1.0, b)
        first = re - im if sa * sb > 0 else re + im
        second = im + re if sa * sb > 0 else im - re
        return first * (sa * abs(a)), second * (sa * abs(a))
    return a * re - b * im, a * im + b * re


def fft_list(load, indices, sign):
    count = len(indices)
    if count == 1:
        return [load(indices[0])]
    even = fft_list(load, indices[0::2], sign)
    odd = fft_list(load, indices[1::2], sign)
    half = count // 2
    low, high = [], []
    for k in range(half):
        t = cmul_const(np.exp(sign * 2j * math.pi * k / count), odd[k])
        low.append((even[k][0] + t[0], even[k][1] + t[1]))
        high.append((even[k][0] - t[0], even[k][1] - t[1]))
    return low + high


PAD = 8


def whole_kernel(
    dims, lam_ref, s_ref, a_ref, re_ref, so_ref, ao_ref,
    r1, hat, src, full, coef, u0, u1, back, outs,
    s_a, r_a, s_b, r_b, s_d, r_d, s_f, r_f, s_r, r_r, s_q, r_q, loc,
):
    groups, slabs, local, depth, nx, ny = dims
    steps = groups * local
    devices = groups * slabs
    nz = depth * slabs
    xb = nx // groups
    rows = xb // 2
    chunks = depth * 2
    t, s = lax.axis_index("tm"), lax.axis_index("space")
    me = t * slabs + s
    half_x = nx // 2
    part = lax.rem(t, 2)
    partner = t + 1 - 2 * part

    def at_chunk(ch):
        return ch // 2, pl.multiple_of(lax.rem(ch, 2) * rows, rows)

    def xrow(block, row, base=0):
        return pl.ds(pl.multiple_of(base + block * xb + row, 8), rows)

    def half():
        return pl.ds(pl.multiple_of(part * half_x, 8), half_x)

    def reaction_send(j):
        s2 = lax.rem(s + j, slabs)
        return pltpu.make_async_remote_copy(
            re_ref.at[:, half(), :], full.at[pl.ds(s * depth, depth), half(), :],
            s_r, r_r, device_id=(t, s2), device_id_type=MESH)

    lax.fori_loop(1, slabs, lambda j, c: (reaction_send(j).start(), c)[1], 0)
    own_reaction = pltpu.make_async_copy(
        re_ref.at[:, half(), :], full.at[pl.ds(s * depth, depth), half(), :], loc.at[0])
    own_reaction.start()

    def a_copy(arr, ch, j):
        z, row = at_chunk(ch)
        t2 = lax.rem(t + j, groups)
        ref = s_ref if arr == 0 else a_ref
        return pltpu.make_async_remote_copy(
            ref.at[:, z, xrow(t2, row), :],
            r1.at[arr, pl.ds(t * local, local), z, pl.ds(row, rows), :],
            s_a.at[ch, arr, j - 1], r_a.at[ch, arr, j - 1],
            device_id=(t2, s), device_id_type=MESH)

    def start_a(ch, c):
        for j in range(1, groups):
            for arr in range(2):
                a_copy(arr, ch, j).start()
        return c

    lax.fori_loop(0, chunks, start_a, 0)
    mine = pl.ds(pl.multiple_of(t * xb, 8), xb)
    own_a = [
        pltpu.make_async_copy(
            ref.at[:, :, mine, :], r1.at[arr, pl.ds(t * local, local)], loc.at[1 + arr])
        for arr, ref in enumerate((s_ref, a_ref))
    ]
    for c in own_a:
        c.start()

    zero = jnp.zeros((nx + 2 * PAD, ny), jnp.float32)
    for buf in (u0, u1):
        def clear(z, c, buf=buf):
            for comp in range(2):
                buf[comp, z] = zero
            return c
        lax.fori_loop(0, nz + 2, clear, 0)
    for c in own_a:
        c.wait()

    growth = [math.exp(math.log(ALPHA) * n / steps) for n in range(steps)]

    def b_copy(ch, j):
        z, row = at_chunk(ch)
        d = lax.rem(me + j, devices)
        return pltpu.make_async_remote_copy(
            hat.at[d, :, z, pl.ds(row, rows), :],
            src.at[:, s * depth + z, xrow(t, row), :],
            s_b, r_b, device_id=(d // slabs, lax.rem(d, slabs)), device_id_type=MESH)

    def forward(ch, c):
        z, row = at_chunk(ch)
        for j in range(1, groups):
            for arr in range(2):
                a_copy(arr, ch, j).wait_recv()

        def piece(r, c):
            at = pl.ds(pl.multiple_of(row + r * 8, 8), 8)

            def load(n):
                return r1[0, n, z, at, :] * growth[n], r1[1, steps - 1 - n, z, at, :] * growth[n]

            for k, (re, im) in enumerate(fft_list(load, list(range(steps)), -1)):
                hat[k, 0, z, at, :] = re
                hat[k, 1, z, at, :] = im
            return c

        lax.fori_loop(0, rows // 8, piece, 0)
        lax.fori_loop(1, devices, lambda j, c: (b_copy(ch, j).start(), c)[1], 0)
        return c

    lax.fori_loop(0, chunks, forward, 0)
    own_b = pltpu.make_async_copy(
        hat.at[me], src.at[:, pl.ds(s * depth, depth), mine, :], loc.at[3])
    own_b.start()

    many = full.at[pl.ds(0, (slabs - 1) * depth), pl.ds(0, half_x), :]
    pltpu.make_async_copy(many, many, r_r).wait()
    own_reaction.wait()
    swap = pltpu.make_async_remote_copy(
        full.at[:, half(), :], full.at[:, half(), :], s_q, r_q,
        device_id=(partner, s), device_id_type=MESH)
    swap.start()
    swap.wait()
    l_re = lam_ref[me, 0] + MU * 6.0
    l_im = lam_ref[me, 1] + BETA

    def coefs(z, c):
        e_re = MU * full[z] + l_re
        inv = 1.0 / (e_re * e_re + l_im * l_im)
        coef[0, z] = e_re * inv
        coef[1, z] = -l_im * inv
        return c

    lax.fori_loop(0, nz, coefs, 0)
    own_b.wait()
    most = hat.at[pl.ds(0, devices - 1)]
    pltpu.make_async_copy(most, most, r_b).wait()

    xc = 32
    lane = lax.broadcasted_iota(jnp.int32, (xc, ny), 1)

    def sweep(cur, new):
        def plane(z, c):
            for x0 in range(0, nx, xc):
                sums = []
                for comp in range(2):
                    total = src[comp, z, x0:x0 + xc, :]
                    if cur is not None:
                        mid = cur[comp, z + 1, PAD + x0:PAD + x0 + xc, :]
                        nb = cur[comp, z + 2, PAD + x0:PAD + x0 + xc, :]
                        nb = nb + cur[comp, z, PAD + x0:PAD + x0 + xc, :]
                        nb = nb + cur[comp, z + 1, PAD + x0 + 1:PAD + x0 + 1 + xc, :]
                        nb = nb + cur[comp, z + 1, PAD + x0 - 1:PAD + x0 - 1 + xc, :]
                        nb = nb + jnp.where(lane == 0, 0.0, pltpu.roll(mid, 1, 1))
                        nb = nb + jnp.where(lane == ny - 1, 0.0, pltpu.roll(mid, ny - 1, 1))
                        total = total + MU * nb
                    sums.append(total)
                c_re = coef[0, z, x0:x0 + xc, :]
                c_im = coef[1, z, x0:x0 + xc, :]
                new[0, z + 1, PAD + x0:PAD + x0 + xc, :] = c_re * sums[0] - c_im * sums[1]
                new[1, z + 1, PAD + x0:PAD + x0 + xc, :] = c_re * sums[1] + c_im * sums[0]
            return c

        lax.fori_loop(0, nz, plane, 0)

    sweep(None, u0)

    def two(i, c):
        sweep(u0, u1)
        sweep(u1, u0)
        return c

    lax.fori_loop(0, (SWEEPS - 1) // 2, two, 0)
    last = u0
    if (SWEEPS - 1) % 2:
        sweep(u0, u1)
        last = u1

    def d_copy(ch, j):
        z, row = at_chunk(ch)
        d = lax.rem(me + j, devices)
        t2, s2 = d // slabs, lax.rem(d, slabs)
        return pltpu.make_async_remote_copy(
            last.at[:, 1 + s2 * depth + z, xrow(t2, row, PAD), :],
            back.at[me, :, z, pl.ds(row, rows), :],
            s_d, r_d.at[ch], device_id=(t2, s2), device_id_type=MESH)

    def start_d(ch, c):
        lax.fori_loop(1, devices, lambda j, c: (d_copy(ch, j).start(), c)[1], 0)
        return c

    lax.fori_loop(0, chunks, start_d, 0)
    own_d = pltpu.make_async_copy(
        last.at[:, pl.ds(1 + s * depth, depth), pl.ds(pl.multiple_of(PAD + t * xb, 8), xb), :],
        back.at[me], loc.at[4])
    own_d.start()
    own_d.wait()
    shrink = [math.exp(-math.log(ALPHA) * n / steps) / steps for n in range(steps)]

    def f_copy(arr, ch, j):
        z, row = at_chunk(ch)
        t2 = lax.rem(t + j, groups)
        ref = so_ref if arr == 0 else ao_ref
        return pltpu.make_async_remote_copy(
            outs.at[arr, pl.ds(t2 * local, local), z, pl.ds(row, rows), :],
            ref.at[:, z, xrow(t, row), :],
            s_f.at[ch, arr, j - 1], r_f.at[ch, arr, j - 1],
            device_id=(t2, s), device_id_type=MESH)

    def backward(ch, c):
        z, row = at_chunk(ch)
        got = back.at[pl.ds(0, devices - 1), :, z, pl.ds(row, rows), :]
        pltpu.make_async_copy(got, got, r_d.at[ch]).wait()

        def piece(r, c):
            at = pl.ds(pl.multiple_of(row + r * 8, 8), 8)

            def load(k):
                return back[k, 0, z, at, :], back[k, 1, z, at, :]

            for n, (re, im) in enumerate(fft_list(load, list(range(steps)), 1)):
                outs[0, n, z, at, :] = re * shrink[n]
                outs[1, steps - 1 - n, z, at, :] = im * shrink[n]
            return c

        lax.fori_loop(0, rows // 8, piece, 0)
        for j in range(1, groups):
            for arr in range(2):
                f_copy(arr, ch, j).start()
        return c

    lax.fori_loop(0, chunks, backward, 0)
    own_f = [
        pltpu.make_async_copy(
            outs.at[arr, pl.ds(t * local, local)], ref.at[:, :, mine, :], loc.at[5 + arr])
        for arr, ref in enumerate((so_ref, ao_ref))
    ]
    for c in own_f:
        c.start()
    for c in own_f:
        c.wait()

    def finish(ch, c):
        for j in range(1, groups):
            for arr in range(2):
                a_copy(arr, ch, j).wait_send()
                f_copy(arr, ch, j).wait()
        return c

    lax.fori_loop(0, chunks, finish, 0)
    pltpu.make_async_copy(most, most, s_b).wait()
    pltpu.make_async_copy(most, most, s_d).wait()
    pltpu.make_async_copy(many, many, s_r).wait()


def fused_body(state_rhs, adjoint_rhs, reaction):
    groups, slabs = lax.axis_size("tm"), lax.axis_size("space")
    local, depth, nx, ny = state_rhs.shape
    dims = (groups, slabs, local, depth, nx, ny)
    steps, devices, nz, xb = groups * local, groups * slabs, depth * slabs, nx // groups
    chunks = depth * 2
    turn = 2.0 * math.pi * np.arange(steps) / steps
    rate = ALPHA ** (1.0 / steps)
    lam = np.stack((1.0 - rate * np.cos(turn), rate * np.sin(turn)), axis=1).astype(np.float32)
    f32 = jnp.float32
    dma = pltpu.SemaphoreType.DMA
    vmem = pl.BlockSpec(memory_space=pltpu.VMEM)
    shape = jax.ShapeDtypeStruct(state_rhs.shape, f32)
    return pl.pallas_call(
        functools.partial(whole_kernel, dims),
        out_shape=(shape, shape),
        in_specs=[pl.BlockSpec(memory_space=pltpu.SMEM), vmem, vmem, vmem],
        out_specs=(vmem, vmem),
        scratch_shapes=[
            pltpu.VMEM((2, steps, depth, xb, ny), f32),
            pltpu.VMEM((devices, 2, depth, xb, ny), f32),
            pltpu.VMEM((2, nz, nx, ny), f32),
            pltpu.VMEM((nz, nx, ny), f32),
            pltpu.VMEM((2, nz, nx, ny), f32),
            pltpu.VMEM((2, nz + 2, nx + 2 * PAD, ny), f32),
            pltpu.VMEM((2, nz + 2, nx + 2 * PAD, ny), f32),
            pltpu.VMEM((devices, 2, depth, xb, ny), f32),
            pltpu.VMEM((2, steps, depth, xb, ny), f32),
            dma((chunks, 2, groups - 1)),
            dma((chunks, 2, groups - 1)),
            dma,
            dma,
            dma,
            dma((chunks,)),
            dma((chunks, 2, groups - 1)),
            dma((chunks, 2, groups - 1)),
            dma,
            dma,
            dma,
            dma,
            dma((7,)),
        ],
        compiler_params=pltpu.CompilerParams(
            has_side_effects=True, vmem_limit_bytes=58 * 1024 * 1024
        ),
    )(jnp.asarray(lam), state_rhs, adjoint_rhs, reaction)


def solution(mesh):
    in_specs = (P("tm", "space", None, None), P("tm", "space", None, None), P("space", None, None))
    out_specs = (P("tm", "space", None, None), P("tm", "space", None, None))
    groups, slabs = mesh.shape["tm"], mesh.shape["space"]

    def chosen(state_rhs, adjoint_rhs, reaction):
        steps = state_rhs.shape[0] * groups
        fits = steps == groups * slabs and steps & (steps - 1) == 0 and groups % 2 == 0
        fits = fits and state_rhs.shape[2] % (16 * groups) == 0 and state_rhs.shape[3] == 128
        return (fused_body if fits else body)(state_rhs, adjoint_rhs, reaction)

    return jax.shard_map(chosen, mesh=mesh, in_specs=in_specs, out_specs=out_specs, check_vma=False)
```

```python
import functools
import math

import jax
import jax.numpy as jnp
import numpy as np
from jax import lax
from jax.experimental import pallas as pl
from jax.experimental.pallas import tpu as pltpu
from jax.sharding import PartitionSpec as P

STEPS = 32
SWEEPS = 12


ALPHA = 0.1
MU = 1.0
BETA = 1.0


def padded_2(cells, sides, width):
    for axis, dim in sides:
        count = lax.axis_size(axis)
        ends = count - 1
        head = lax.slice_in_dim(cells, 0, width, axis=dim)
        tail = lax.slice_in_dim(cells, cells.shape[dim] - width, cells.shape[dim], axis=dim)
        cells = jnp.concatenate(
            [
                lax.ppermute(tail, axis, [(i, (i + 1) % count) for i in range(ends)]),
                cells,
                lax.ppermute(head, axis, [((i + 1) % count, i) for i in range(ends)]),
            ],
            axis=dim,
        )
    return cells


def coefficients(reaction, freqs):
    turn = 2.0 * math.pi * freqs.astype(jnp.float32) / STEPS
    rate = math.exp(math.log(ALPHA) / STEPS)
    lam_re = 1.0 - rate * jnp.cos(turn)
    lam_im = rate * jnp.sin(turn)
    shaped = (-1,) + (1,) * reaction.ndim
    d_re = lam_re.reshape(shaped) + MU * (6.0 + reaction)
    d_im = jnp.broadcast_to(lam_im.reshape(shaped), d_re.shape)
    den_re = d_re * d_re - d_im * d_im + BETA * BETA
    den_im = 2.0 * d_re * d_im
    magnitude = den_re * den_re + den_im * den_im
    inv_re = den_re / magnitude
    inv_im = -den_im / magnitude
    return (
        d_re * inv_re - d_im * inv_im,
        d_re * inv_im + d_im * inv_re,
        BETA * inv_re,
        BETA * inv_im,
    )


def block_solve(coefficient, source):
    q_re, q_im, r_re, r_im = coefficient
    y_real = source[..., 0, :, :, :]
    y_imag = source[..., 1, :, :, :]
    p_real = source[..., 2, :, :, :]
    p_imag = source[..., 3, :, :, :]
    new_yre = q_re * y_real - q_im * y_imag + (r_re * p_real - r_im * p_imag)
    new_yim = q_re * y_imag + q_im * y_real + (r_re * p_imag + r_im * p_real)
    new_pre = q_re * p_real - q_im * p_imag - (r_re * y_real - r_im * y_imag)
    new_pim = q_re * p_imag + q_im * p_real - (r_re * y_imag + r_im * y_real)
    return jnp.stack((new_yre, new_yim, new_pre, new_pim), axis=-4)


def neighbour_sum(zpadded):
    inner = zpadded[:, :, 1:-1]
    padded = jnp.pad(inner, ((0, 0), (0, 0), (0, 0), (1, 1), (1, 1)))
    total = zpadded[:, :, 2:] + zpadded[:, :, :-2]
    total = total + padded[:, :, :, 2:, 1:-1] + padded[:, :, :, :-2, 1:-1]
    return total + padded[:, :, :, 1:-1, 2:] + padded[:, :, :, 1:-1, :-2]


def effective(times, reverse):
    if reverse:
        return STEPS - 1 - times
    return times


def forward_table(freqs, times, reverse):
    moment = effective(times, reverse)
    phase = freqs[:, None] * moment[None, :] % STEPS
    angle = 2.0 * math.pi / STEPS * phase.astype(jnp.float32)
    growth = jnp.exp(math.log(ALPHA) * moment.astype(jnp.float32) / STEPS)[None, :]
    table = jnp.stack((jnp.cos(angle) * growth, -jnp.sin(angle) * growth), axis=1)
    return table.reshape(-1, times.shape[0])


def inverse_table(freqs, times, reverse):
    moment = effective(times, reverse)
    phase = moment[:, None] * freqs[None, :] % STEPS
    angle = 2.0 * math.pi / STEPS * phase.astype(jnp.float32)
    shrink = jnp.exp(-math.log(ALPHA) * moment.astype(jnp.float32) / STEPS)[:, None] / STEPS
    table = jnp.stack((jnp.cos(angle) * shrink, -jnp.sin(angle) * shrink), axis=2)
    return table.reshape(times.shape[0], -1)


def forward_pair(state_part, adjoint_part, freqs, times):
    rows = state_part.shape[0]
    state_hat = jnp.dot(
        forward_table(freqs, times, False),
        state_part.reshape(rows, -1),
        precision=lax.Precision.HIGHEST,
    )
    adjoint_hat = jnp.dot(
        forward_table(freqs, times, True),
        adjoint_part.reshape(rows, -1),
        precision=lax.Precision.HIGHEST,
    )
    return (state_hat, adjoint_hat)


def backward_pair(solved, freqs, times):
    count = solved.shape[0]
    slab = solved.shape[2:]
    flat_state = solved[:, 0:2].reshape(2 * count, -1)
    flat_adjoint = solved[:, 2:4].reshape(2 * count, -1)
    state_time = jnp.dot(
        inverse_table(freqs, times, False), flat_state, precision=lax.Precision.HIGHEST
    )
    adjoint_time = jnp.dot(
        inverse_table(freqs, times, True), flat_adjoint, precision=lax.Precision.HIGHEST
    )
    shaped = (times.shape[0],) + slab
    return (state_time.reshape(shaped), adjoint_time.reshape(shaped))


def body(state_rhs, adjoint_rhs, reaction):
    groups = lax.axis_size("tm")
    local_steps = state_rhs.shape[0]
    freq_count = STEPS // groups
    slab_shape = state_rhs.shape[1:]
    freqs = lax.axis_index("tm") * freq_count + jnp.arange(freq_count, dtype=jnp.int32)
    pieces = (
        lax.all_gather(state_rhs, "tm", axis=0, tiled=True),
        lax.all_gather(adjoint_rhs, "tm", axis=0, tiled=True),
    )
    rows = pieces[0].shape[0]
    times = jnp.arange(rows, dtype=jnp.int32)
    state_hat, adjoint_hat = forward_pair(pieces[0], pieces[1], freqs, times)
    state_hat, adjoint_hat = (state_hat, adjoint_hat)
    sources = jnp.concatenate(
        (
            state_hat.reshape((freq_count, 2) + slab_shape),
            adjoint_hat.reshape((freq_count, 2) + slab_shape),
        ),
        axis=1,
    )
    coefficient = coefficients(reaction, freqs)
    field = block_solve(coefficient, sources)

    def sweep(sweep_index, current):
        zpadded = padded_2(current, (("space", 2),), 1)
        return block_solve(coefficient, sources + MU * neighbour_sum(zpadded))

    solved = lax.fori_loop(0, SWEEPS - 1, sweep, field)
    times = jnp.arange(local_steps * lax.axis_size("tm"), dtype=jnp.int32)
    state_time, adjoint_time = backward_pair(solved, freqs, times)
    combined = lax.psum_scatter(
        jnp.stack((state_time, adjoint_time), axis=1), "tm", scatter_dimension=0, tiled=True
    )
    state_out = combined[:, 0]
    adjoint_out = combined[:, 1]
    return (state_out, adjoint_out)


MESH = pl.DeviceIdType.MESH


def cmul_const(factor, value):
    re, im = value
    a, b = float(factor.real), float(factor.imag)
    if abs(b) < 1e-12 and abs(a - 1.0) < 1e-12:
        return value
    if abs(a) < 1e-12:
        return (-im, re) if b > 0 else (im, -re)
    if abs(abs(a) - abs(b)) < 1e-12:
        sa, sb = math.copysign(1.0, a), math.copysign(1.0, b)
        first = re - im if sa * sb > 0 else re + im
        second = im + re if sa * sb > 0 else im - re
        return first * (sa * abs(a)), second * (sa * abs(a))
    return a * re - b * im, a * im + b * re


def fft_list(load, indices, sign):
    count = len(indices)
    if count == 1:
        return [load(indices[0])]
    even = fft_list(load, indices[0::2], sign)
    odd = fft_list(load, indices[1::2], sign)
    half = count // 2
    low, high = [], []
    for k in range(half):
        t = cmul_const(np.exp(sign * 2j * math.pi * k / count), odd[k])
        low.append((even[k][0] + t[0], even[k][1] + t[1]))
        high.append((even[k][0] - t[0], even[k][1] - t[1]))
    return low + high


LOW, HIGH = 16, 24


def whole_kernel(
    dims, lam_ref, s_ref, a_ref, re_ref, so_ref, ao_ref,
    r1, hat, src, full, coef, u0, u1, back, outs,
    s_a, r_a, s_b, r_b, s_d, r_d, s_f, r_f, s_r, r_r, s_y, r_y, s_q, r_q, loc,
):
    groups, slabs, local, depth, nx, ny = dims
    steps = groups * local
    devices = groups * slabs
    nz = depth * slabs
    xb = nx // groups
    rows = 8
    chunks = xb // rows
    xstep = nx // chunks
    t, s = lax.axis_index("tm"), lax.axis_index("space")
    me = t * slabs + s
    half_x = nx // 2
    part = lax.rem(t, 2)
    partner = t + 1 - 2 * part

    def kept(ch):
        return pl.ds(pl.multiple_of(ch * rows, rows), rows)

    def xrow(ch, member, base=0):
        return pl.ds(pl.multiple_of(base + ch * xstep + member * rows, rows), rows)

    def half():
        return pl.ds(pl.multiple_of(part * half_x, 8), half_x)

    def reaction_send(j):
        s2 = lax.rem(s + 2 * j, slabs)
        return pltpu.make_async_remote_copy(
            re_ref.at[:, half(), :], full.at[pl.ds(s * depth, depth), half(), :],
            s_r, r_r, device_id=(t, s2), device_id_type=MESH)

    parity = lax.rem(s, 2)

    def parity_send(i):
        planes = full.at[pl.ds((2 * i + parity) * depth, depth), half(), :]
        return pltpu.make_async_remote_copy(
            planes, planes, s_y, r_y, device_id=(t, s + 1 - 2 * parity), device_id_type=MESH)

    def planes_of(count):
        return full.at[pl.ds(0, count * depth), pl.ds(0, half_x), :]

    def wait_bytes(ref, sem):
        pltpu.make_async_copy(ref, ref, sem).wait()

    for j in range(1, slabs // 2):
        reaction_send(j).start()
    own_reaction = pltpu.make_async_copy(
        re_ref.at[:, half(), :], full.at[pl.ds(s * depth, depth), half(), :], loc.at[0, 0, 0])
    own_reaction.start()

    def a_copy(arr, ch, j):
        t2 = lax.rem(t + j, groups)
        ref = s_ref if arr == 0 else a_ref
        return pltpu.make_async_remote_copy(
            ref.at[:, :, xrow(ch, t2), :],
            r1.at[arr, pl.ds(t * local, local), :, kept(ch), :],
            s_a.at[ch, arr, j - 1], r_a.at[ch, arr, j - 1],
            device_id=(t2, s), device_id_type=MESH)

    def start_a(ch, c):
        for j in range(1, groups):
            for arr in range(2):
                a_copy(arr, ch, j).start()
        return c

    lax.fori_loop(0, chunks, start_a, 0)
    own_a = [
        pltpu.make_async_copy(
            ref.at[:, :, xrow(ch, t), :],
            r1.at[arr, pl.ds(t * local, local), :, kept(ch), :], loc.at[1, arr, ch])
        for arr, ref in enumerate((s_ref, a_ref))
        for ch in range(chunks)
    ]
    for c in own_a:
        c.start()

    zero = jnp.zeros((LOW + nx + HIGH, ny), jnp.float32)
    for buf, extra in ((u0, 2), (u1, 2)):
        def clear(z, c, buf=buf):
            for comp in range(2):
                buf[comp, z] = zero
            return c
        lax.fori_loop(0, nz + extra, clear, 0)

    def clear_edges(z, c):
        for buf in (src, coef):
            for comp in range(2):
                buf[comp, z, 0:LOW, :] = zero[0:LOW]
                buf[comp, z, LOW + nx:, :] = zero[0:HIGH]
        return c

    lax.fori_loop(0, nz, clear_edges, 0)
    for c in own_a:
        c.wait()

    growth = [math.exp(math.log(ALPHA) * n / steps) for n in range(steps)]

    def b_copy(ch, j):
        d = lax.rem(me + j, devices)
        return pltpu.make_async_remote_copy(
            hat.at[d, :, :, kept(ch), :],
            src.at[:, pl.ds(s * depth, depth), xrow(ch, t, LOW), :],
            s_b, r_b.at[ch], device_id=(d // slabs, lax.rem(d, slabs)), device_id_type=MESH)

    def own_b(ch):
        return pltpu.make_async_copy(
            hat.at[me, :, :, kept(ch), :],
            src.at[:, pl.ds(s * depth, depth), xrow(ch, t, LOW), :], loc.at[2, 0, ch])

    def forward(ch, c):
        for j in range(1, groups):
            for arr in range(2):
                a_copy(arr, ch, j).wait_recv()

        def piece(z, c):
            at = kept(ch)

            def load(n):
                return r1[0, n, z, at, :] * growth[n], r1[1, steps - 1 - n, z, at, :] * growth[n]

            for k, (re, im) in enumerate(fft_list(load, list(range(steps)), -1)):
                hat[k, 0, z, at, :] = re
                hat[k, 1, z, at, :] = im
            return c

        lax.fori_loop(0, depth, piece, 0)
        lax.fori_loop(1, devices, lambda j, c: (b_copy(ch, j).start(), c)[1], 0)
        own_b(ch).start()
        return c

    lax.fori_loop(0, 1, forward, 0)
    wait_bytes(planes_of(slabs // 2 - 1), r_r)
    own_reaction.wait()
    for i in range(slabs // 2):
        parity_send(i).start()
    lax.fori_loop(1, chunks, forward, 0)

    wait_bytes(planes_of(slabs // 2), r_y)
    swap = pltpu.make_async_remote_copy(
        full.at[:, half(), :], full.at[:, half(), :], s_q, r_q,
        device_id=(partner, s), device_id_type=MESH)
    swap.start()
    swap.wait()
    l_re = lam_ref[me, 0] + MU * 6.0
    l_im = lam_ref[me, 1] + BETA

    def coefs(z, c):
        e_re = MU * full[z] + l_re
        inv = 1.0 / (e_re * e_re + l_im * l_im)
        coef[0, z, LOW:LOW + nx, :] = e_re * inv
        coef[1, z, LOW:LOW + nx, :] = -l_im * inv
        return c

    lax.fori_loop(0, nz, coefs, 0)

    def tile(c, j, width):
        x0 = LOW + c * xstep - j
        cur, new = (u0, u1) if j % 2 else (u1, u0)
        lane = lax.broadcasted_iota(jnp.int32, (width, ny), 1)

        def plane(z, carry):
            sums = []
            for comp in range(2):
                total = src[comp, z, x0:x0 + width, :]
                if j > 0:
                    mid = cur[comp, z + 1, x0:x0 + width, :]
                    nb = cur[comp, z + 2, x0:x0 + width, :]
                    nb = nb + cur[comp, z, x0:x0 + width, :]
                    nb = nb + cur[comp, z + 1, x0 + 1:x0 + 1 + width, :]
                    nb = nb + cur[comp, z + 1, x0 - 1:x0 - 1 + width, :]
                    nb = nb + jnp.where(lane == 0, 0.0, pltpu.roll(mid, 1, 1))
                    nb = nb + jnp.where(lane == ny - 1, 0.0, pltpu.roll(mid, ny - 1, 1))
                    total = total + MU * nb
                sums.append(total)
            c_re = coef[0, z, x0:x0 + width, :]
            c_im = coef[1, z, x0:x0 + width, :]
            new[0, z + 1, x0:x0 + width, :] = c_re * sums[0] - c_im * sums[1]
            new[1, z + 1, x0:x0 + width, :] = c_re * sums[1] + c_im * sums[0]
            return carry

        lax.fori_loop(0, nz, plane, 0, unroll=2)

    last = u0 if SWEEPS % 2 else u1

    def d_copy(ch, j):
        d = lax.rem(me + j, devices)
        t2, s2 = d // slabs, lax.rem(d, slabs)
        return pltpu.make_async_remote_copy(
            last.at[:, pl.ds(1 + s2 * depth, depth), xrow(ch, t2, LOW), :],
            back.at[me, :, :, kept(ch), :],
            s_d, r_d.at[ch], device_id=(t2, s2), device_id_type=MESH)

    def own_d(ch):
        return pltpu.make_async_copy(
            last.at[:, pl.ds(1 + s * depth, depth), xrow(ch, t, LOW), :],
            back.at[me, :, :, kept(ch), :], loc.at[3, 0, ch])

    def others(ch):
        return hat.at[pl.ds(0, devices - 1), :, :, kept(ch), :]

    for c in range(chunks + 1):
        if c < chunks:
            own_b(c).wait()
            wait_bytes(others(c), r_b.at[c])
        for j in range(SWEEPS):
            tile(c, j, xstep if c < chunks else LOW)
        if c > 0:
            lax.fori_loop(1, devices, lambda j, k, c=c: (d_copy(c - 1, j).start(), k)[1], 0)
            own_d(c - 1).start()
    shrink = [math.exp(-math.log(ALPHA) * n / steps) / steps for n in range(steps)]

    def f_copy(arr, ch, j):
        t2 = lax.rem(t + j, groups)
        ref = so_ref if arr == 0 else ao_ref
        return pltpu.make_async_remote_copy(
            outs.at[arr, pl.ds(t2 * local, local), :, kept(ch), :],
            ref.at[:, :, xrow(ch, t), :],
            s_f.at[ch, arr, j - 1], r_f.at[ch, arr, j - 1],
            device_id=(t2, s), device_id_type=MESH)

    def own_f(arr, ch):
        ref = so_ref if arr == 0 else ao_ref
        return pltpu.make_async_copy(
            outs.at[arr, pl.ds(t * local, local), :, kept(ch), :],
            ref.at[:, :, xrow(ch, t), :], loc.at[4, arr, ch])

    def backward(ch, c):
        wait_bytes(others(ch), r_d.at[ch])
        own_d(ch).wait()

        def piece(z, c):
            at = kept(ch)

            def load(k):
                return back[k, 0, z, at, :], back[k, 1, z, at, :]

            for n, (re, im) in enumerate(fft_list(load, list(range(steps)), 1)):
                outs[0, n, z, at, :] = re * shrink[n]
                outs[1, steps - 1 - n, z, at, :] = im * shrink[n]
            return c

        lax.fori_loop(0, depth, piece, 0)
        for arr in range(2):
            for j in range(1, groups):
                f_copy(arr, ch, j).start()
            own_f(arr, ch).start()
        return c

    lax.fori_loop(0, chunks, backward, 0)
    def finish(ch, c):
        for j in range(1, groups):
            for arr in range(2):
                a_copy(arr, ch, j).wait_send()
                f_copy(arr, ch, j).wait()
        for arr in range(2):
            own_f(arr, ch).wait()
        return c

    lax.fori_loop(0, chunks, finish, 0)
    most = hat.at[pl.ds(0, devices - 1)]
    wait_bytes(most, s_b)
    wait_bytes(most, s_d)
    wait_bytes(planes_of(slabs // 2 - 1), s_r)
    wait_bytes(planes_of(slabs // 2), s_y)


def fused_body(state_rhs, adjoint_rhs, reaction):
    groups, slabs = lax.axis_size("tm"), lax.axis_size("space")
    local, depth, nx, ny = state_rhs.shape
    dims = (groups, slabs, local, depth, nx, ny)
    steps, devices, nz, xb = groups * local, groups * slabs, depth * slabs, nx // groups
    chunks = xb // 8
    edged = LOW + nx + HIGH
    turn = 2.0 * math.pi * np.arange(steps) / steps
    rate = ALPHA ** (1.0 / steps)
    lam = np.stack((1.0 - rate * np.cos(turn), rate * np.sin(turn)), axis=1).astype(np.float32)
    f32 = jnp.float32
    dma = pltpu.SemaphoreType.DMA
    vmem = pl.BlockSpec(memory_space=pltpu.VMEM)
    shape = jax.ShapeDtypeStruct(state_rhs.shape, f32)
    return pl.pallas_call(
        functools.partial(whole_kernel, dims),
        out_shape=(shape, shape),
        in_specs=[pl.BlockSpec(memory_space=pltpu.SMEM), vmem, vmem, vmem],
        out_specs=(vmem, vmem),
        scratch_shapes=[
            pltpu.VMEM((2, steps, depth, xb, ny), f32),
            pltpu.VMEM((devices, 2, depth, xb, ny), f32),
            pltpu.VMEM((2, nz, edged, ny), f32),
            pltpu.VMEM((nz, nx, ny), f32),
            pltpu.VMEM((2, nz, edged, ny), f32),
            pltpu.VMEM((2, nz + 2, edged, ny), f32),
            pltpu.VMEM((2, nz + 2, edged, ny), f32),
            pltpu.VMEM((devices, 2, depth, xb, ny), f32),
            pltpu.VMEM((2, steps, depth, xb, ny), f32),
            dma((chunks, 2, groups - 1)),
            dma((chunks, 2, groups - 1)),
            dma,
            dma((chunks,)),
            dma,
            dma((chunks,)),
            dma((chunks, 2, groups - 1)),
            dma((chunks, 2, groups - 1)),
            dma,
            dma,
            dma,
            dma,
            dma,
            dma,
            dma((5, 2, chunks)),
        ],
        compiler_params=pltpu.CompilerParams(
            has_side_effects=True, vmem_limit_bytes=58 * 1024 * 1024
        ),
    )(jnp.asarray(lam), state_rhs, adjoint_rhs, reaction)


def solution(mesh):
    in_specs = (P("tm", "space", None, None), P("tm", "space", None, None), P("space", None, None))
    out_specs = (P("tm", "space", None, None), P("tm", "space", None, None))
    groups, slabs = mesh.shape["tm"], mesh.shape["space"]

    def chosen(state_rhs, adjoint_rhs, reaction):
        steps = state_rhs.shape[0] * groups
        fits = steps == groups * slabs and steps & (steps - 1) == 0 and groups % 2 == 0
        fits = fits and slabs % 2 == 0 and slabs > 2 and state_rhs.shape[3] % 128 == 0
        fits = fits and state_rhs.shape[2] % (8 * groups) == 0 and SWEEPS <= LOW <= 8 * groups
        return (fused_body if fits else body)(state_rhs, adjoint_rhs, reaction)

    return jax.shard_map(chosen, mesh=mesh, in_specs=in_specs, out_specs=out_specs, check_vma=False)
```

```python
import functools
import math

import jax
import jax.numpy as jnp
import numpy as np
from jax import lax
from jax.experimental import pallas as pl
from jax.experimental.pallas import tpu as pltpu
from jax.sharding import PartitionSpec as P

STEPS = 32
SWEEPS = 12


ALPHA = 0.1
MU = 1.0
BETA = 1.0


def padded_2(cells, sides, width):
    for axis, dim in sides:
        count = lax.axis_size(axis)
        ends = count - 1
        head = lax.slice_in_dim(cells, 0, width, axis=dim)
        tail = lax.slice_in_dim(cells, cells.shape[dim] - width, cells.shape[dim], axis=dim)
        cells = jnp.concatenate(
            [
                lax.ppermute(tail, axis, [(i, (i + 1) % count) for i in range(ends)]),
                cells,
                lax.ppermute(head, axis, [((i + 1) % count, i) for i in range(ends)]),
            ],
            axis=dim,
        )
    return cells


def coefficients(reaction, freqs):
    turn = 2.0 * math.pi * freqs.astype(jnp.float32) / STEPS
    rate = math.exp(math.log(ALPHA) / STEPS)
    lam_re = 1.0 - rate * jnp.cos(turn)
    lam_im = rate * jnp.sin(turn)
    shaped = (-1,) + (1,) * reaction.ndim
    d_re = lam_re.reshape(shaped) + MU * (6.0 + reaction)
    d_im = jnp.broadcast_to(lam_im.reshape(shaped), d_re.shape)
    den_re = d_re * d_re - d_im * d_im + BETA * BETA
    den_im = 2.0 * d_re * d_im
    magnitude = den_re * den_re + den_im * den_im
    inv_re = den_re / magnitude
    inv_im = -den_im / magnitude
    return (
        d_re * inv_re - d_im * inv_im,
        d_re * inv_im + d_im * inv_re,
        BETA * inv_re,
        BETA * inv_im,
    )


def block_solve(coefficient, source):
    q_re, q_im, r_re, r_im = coefficient
    y_real = source[..., 0, :, :, :]
    y_imag = source[..., 1, :, :, :]
    p_real = source[..., 2, :, :, :]
    p_imag = source[..., 3, :, :, :]
    new_yre = q_re * y_real - q_im * y_imag + (r_re * p_real - r_im * p_imag)
    new_yim = q_re * y_imag + q_im * y_real + (r_re * p_imag + r_im * p_real)
    new_pre = q_re * p_real - q_im * p_imag - (r_re * y_real - r_im * y_imag)
    new_pim = q_re * p_imag + q_im * p_real - (r_re * y_imag + r_im * y_real)
    return jnp.stack((new_yre, new_yim, new_pre, new_pim), axis=-4)


def neighbour_sum(zpadded):
    inner = zpadded[:, :, 1:-1]
    padded = jnp.pad(inner, ((0, 0), (0, 0), (0, 0), (1, 1), (1, 1)))
    total = zpadded[:, :, 2:] + zpadded[:, :, :-2]
    total = total + padded[:, :, :, 2:, 1:-1] + padded[:, :, :, :-2, 1:-1]
    return total + padded[:, :, :, 1:-1, 2:] + padded[:, :, :, 1:-1, :-2]


def effective(times, reverse):
    if reverse:
        return STEPS - 1 - times
    return times


def forward_table(freqs, times, reverse):
    moment = effective(times, reverse)
    phase = freqs[:, None] * moment[None, :] % STEPS
    angle = 2.0 * math.pi / STEPS * phase.astype(jnp.float32)
    growth = jnp.exp(math.log(ALPHA) * moment.astype(jnp.float32) / STEPS)[None, :]
    table = jnp.stack((jnp.cos(angle) * growth, -jnp.sin(angle) * growth), axis=1)
    return table.reshape(-1, times.shape[0])


def inverse_table(freqs, times, reverse):
    moment = effective(times, reverse)
    phase = moment[:, None] * freqs[None, :] % STEPS
    angle = 2.0 * math.pi / STEPS * phase.astype(jnp.float32)
    shrink = jnp.exp(-math.log(ALPHA) * moment.astype(jnp.float32) / STEPS)[:, None] / STEPS
    table = jnp.stack((jnp.cos(angle) * shrink, -jnp.sin(angle) * shrink), axis=2)
    return table.reshape(times.shape[0], -1)


def forward_pair(state_part, adjoint_part, freqs, times):
    rows = state_part.shape[0]
    state_hat = jnp.dot(
        forward_table(freqs, times, False),
        state_part.reshape(rows, -1),
        precision=lax.Precision.HIGHEST,
    )
    adjoint_hat = jnp.dot(
        forward_table(freqs, times, True),
        adjoint_part.reshape(rows, -1),
        precision=lax.Precision.HIGHEST,
    )
    return (state_hat, adjoint_hat)


def backward_pair(solved, freqs, times):
    count = solved.shape[0]
    slab = solved.shape[2:]
    flat_state = solved[:, 0:2].reshape(2 * count, -1)
    flat_adjoint = solved[:, 2:4].reshape(2 * count, -1)
    state_time = jnp.dot(
        inverse_table(freqs, times, False), flat_state, precision=lax.Precision.HIGHEST
    )
    adjoint_time = jnp.dot(
        inverse_table(freqs, times, True), flat_adjoint, precision=lax.Precision.HIGHEST
    )
    shaped = (times.shape[0],) + slab
    return (state_time.reshape(shaped), adjoint_time.reshape(shaped))


def body(state_rhs, adjoint_rhs, reaction):
    groups = lax.axis_size("tm")
    local_steps = state_rhs.shape[0]
    freq_count = STEPS // groups
    slab_shape = state_rhs.shape[1:]
    freqs = lax.axis_index("tm") * freq_count + jnp.arange(freq_count, dtype=jnp.int32)
    pieces = (
        lax.all_gather(state_rhs, "tm", axis=0, tiled=True),
        lax.all_gather(adjoint_rhs, "tm", axis=0, tiled=True),
    )
    rows = pieces[0].shape[0]
    times = jnp.arange(rows, dtype=jnp.int32)
    state_hat, adjoint_hat = forward_pair(pieces[0], pieces[1], freqs, times)
    state_hat, adjoint_hat = (state_hat, adjoint_hat)
    sources = jnp.concatenate(
        (
            state_hat.reshape((freq_count, 2) + slab_shape),
            adjoint_hat.reshape((freq_count, 2) + slab_shape),
        ),
        axis=1,
    )
    coefficient = coefficients(reaction, freqs)
    field = block_solve(coefficient, sources)

    def sweep(sweep_index, current):
        zpadded = padded_2(current, (("space", 2),), 1)
        return block_solve(coefficient, sources + MU * neighbour_sum(zpadded))

    solved = lax.fori_loop(0, SWEEPS - 1, sweep, field)
    times = jnp.arange(local_steps * lax.axis_size("tm"), dtype=jnp.int32)
    state_time, adjoint_time = backward_pair(solved, freqs, times)
    combined = lax.psum_scatter(
        jnp.stack((state_time, adjoint_time), axis=1), "tm", scatter_dimension=0, tiled=True
    )
    state_out = combined[:, 0]
    adjoint_out = combined[:, 1]
    return (state_out, adjoint_out)


MESH = pl.DeviceIdType.MESH


def cmul_const(factor, value):
    re, im = value
    a, b = float(factor.real), float(factor.imag)
    if abs(b) < 1e-12 and abs(a - 1.0) < 1e-12:
        return value
    if abs(a) < 1e-12:
        return (-im, re) if b > 0 else (im, -re)
    if abs(abs(a) - abs(b)) < 1e-12:
        sa, sb = math.copysign(1.0, a), math.copysign(1.0, b)
        first = re - im if sa * sb > 0 else re + im
        second = im + re if sa * sb > 0 else im - re
        return first * (sa * abs(a)), second * (sa * abs(a))
    return a * re - b * im, a * im + b * re


def fft_list(load, indices, sign):
    count = len(indices)
    if count == 1:
        return [load(indices[0])]
    even = fft_list(load, indices[0::2], sign)
    odd = fft_list(load, indices[1::2], sign)
    half = count // 2
    low, high = [], []
    for k in range(half):
        t = cmul_const(np.exp(sign * 2j * math.pi * k / count), odd[k])
        low.append((even[k][0] + t[0], even[k][1] + t[1]))
        high.append((even[k][0] - t[0], even[k][1] - t[1]))
    return low + high


LOW, HIGH = 16, 24


def whole_kernel(
    dims, lam_ref, s_ref, a_ref, re_ref, so_ref, ao_ref,
    r1, hat, src, full, coef, u0, u1, back, outs,
    s_a, r_a, s_b, r_b, s_d, r_d, s_f, r_f, s_r, r_r, s_y, r_y, s_q, r_q, loc,
):
    groups, slabs, local, depth, nx, ny = dims
    steps = groups * local
    devices = groups * slabs
    nz = depth * slabs
    xb = nx // groups
    rows = 8
    chunks = xb // rows
    xstep = nx // chunks
    t, s = lax.axis_index("tm"), lax.axis_index("space")
    me = t * slabs + s
    half_x = nx // 2
    part = lax.rem(t, 2)
    partner = t + 1 - 2 * part

    bits = devices.bit_length() - 1
    order = sorted(range(1, devices), key=lambda j: (-((j >> 2) & 1), -((j >> 1) & 1), -((j >> 4) & 1), -j))
    flip = [lax.rem(me // (1 << b), 2) for b in range(bits)]

    def across(j):
        d = me
        for b in range(bits):
            if (j >> b) & 1:
                d = d + (1 << b) * (1 - 2 * flip[b])
        return d

    def kept(ch):
        return pl.ds(pl.multiple_of(ch * rows, rows), rows)

    def xrow(ch, member, base=0):
        return pl.ds(pl.multiple_of(base + ch * xstep + member * rows, rows), rows)

    def half():
        return pl.ds(pl.multiple_of(part * half_x, 8), half_x)

    def reaction_send(j):
        s2 = lax.rem(s + 2 * j, slabs)
        return pltpu.make_async_remote_copy(
            re_ref.at[:, half(), :], full.at[pl.ds(s * depth, depth), half(), :],
            s_r, r_r, device_id=(t, s2), device_id_type=MESH)

    parity = lax.rem(s, 2)

    def parity_send(i):
        planes = full.at[pl.ds((2 * i + parity) * depth, depth), half(), :]
        return pltpu.make_async_remote_copy(
            planes, planes, s_y, r_y, device_id=(t, s + 1 - 2 * parity), device_id_type=MESH)

    def planes_of(count):
        return full.at[pl.ds(0, count * depth), pl.ds(0, half_x), :]

    def wait_bytes(ref, sem):
        pltpu.make_async_copy(ref, ref, sem).wait()

    for j in range(1, slabs // 2):
        reaction_send(j).start()
    own_reaction = pltpu.make_async_copy(
        re_ref.at[:, half(), :], full.at[pl.ds(s * depth, depth), half(), :], loc.at[0, 0, 0])
    own_reaction.start()

    def a_copy(arr, ch, j):
        t2 = lax.rem(t + j, groups)
        ref = s_ref if arr == 0 else a_ref
        return pltpu.make_async_remote_copy(
            ref.at[:, :, xrow(ch, t2), :],
            r1.at[arr, pl.ds(t * local, local), :, kept(ch), :],
            s_a.at[ch, arr, j - 1], r_a.at[ch, arr, j - 1],
            device_id=(t2, s), device_id_type=MESH)

    def start_a(ch, c):
        for j in range(1, groups):
            for arr in range(2):
                a_copy(arr, ch, j).start()
        return c

    lax.fori_loop(0, chunks, start_a, 0)
    own_a = [
        pltpu.make_async_copy(
            ref.at[:, :, xrow(ch, t), :],
            r1.at[arr, pl.ds(t * local, local), :, kept(ch), :], loc.at[1, arr, ch])
        for arr, ref in enumerate((s_ref, a_ref))
        for ch in range(chunks)
    ]
    for c in own_a:
        c.start()

    zero = jnp.zeros((LOW + nx + HIGH, ny), jnp.float32)
    for buf, extra in ((u0, 2), (u1, 2)):
        def clear(z, c, buf=buf):
            for comp in range(2):
                buf[comp, z] = zero
            return c
        lax.fori_loop(0, nz + extra, clear, 0)

    def clear_edges(z, c):
        for buf in (src, coef):
            for comp in range(2):
                buf[comp, z, 0:LOW, :] = zero[0:LOW]
                buf[comp, z, LOW + nx:, :] = zero[0:HIGH]
        return c

    lax.fori_loop(0, nz, clear_edges, 0)
    for c in own_a:
        c.wait()

    growth = [math.exp(math.log(ALPHA) * n / steps) for n in range(steps)]

    def b_copy(ch, j):
        d = across(j)
        return pltpu.make_async_remote_copy(
            hat.at[d, :, :, kept(ch), :],
            src.at[:, pl.ds(s * depth, depth), xrow(ch, t, LOW), :],
            s_b, r_b.at[ch], device_id=(d // slabs, lax.rem(d, slabs)), device_id_type=MESH)

    def own_b(ch):
        return pltpu.make_async_copy(
            hat.at[me, :, :, kept(ch), :],
            src.at[:, pl.ds(s * depth, depth), xrow(ch, t, LOW), :], loc.at[2, 0, ch])

    def forward(ch, c):
        for j in range(1, groups):
            for arr in range(2):
                a_copy(arr, ch, j).wait_recv()

        def piece(z, c):
            at = kept(ch)

            def load(n):
                return r1[0, n, z, at, :] * growth[n], r1[1, steps - 1 - n, z, at, :] * growth[n]

            for k, (re, im) in enumerate(fft_list(load, list(range(steps)), -1)):
                hat[k, 0, z, at, :] = re
                hat[k, 1, z, at, :] = im
            return c

        lax.fori_loop(0, depth, piece, 0)
        for j in order:
            b_copy(ch, j).start()
        own_b(ch).start()
        return c

    lax.fori_loop(0, 1, forward, 0)
    wait_bytes(planes_of(slabs // 2 - 1), r_r)
    own_reaction.wait()
    for i in range(slabs // 2):
        parity_send(i).start()
    lax.fori_loop(1, chunks, forward, 0)

    wait_bytes(planes_of(slabs // 2), r_y)
    swap = pltpu.make_async_remote_copy(
        full.at[:, half(), :], full.at[:, half(), :], s_q, r_q,
        device_id=(partner, s), device_id_type=MESH)
    swap.start()
    swap.wait()
    l_re = lam_ref[me, 0] + MU * 6.0
    l_im = lam_ref[me, 1] + BETA

    def coefs(z, c):
        e_re = MU * full[z] + l_re
        inv = 1.0 / (e_re * e_re + l_im * l_im)
        coef[0, z, LOW:LOW + nx, :] = e_re * inv
        coef[1, z, LOW:LOW + nx, :] = -l_im * inv
        return c

    lax.fori_loop(0, nz, coefs, 0)

    def tile(c, j, width):
        x0 = LOW + c * xstep - j
        cur, new = (u0, u1) if j % 2 else (u1, u0)
        lane = lax.broadcasted_iota(jnp.int32, (width, ny), 1)

        def plane(z, carry):
            sums = []
            for comp in range(2):
                total = src[comp, z, x0:x0 + width, :]
                if j > 0:
                    mid = cur[comp, z + 1, x0:x0 + width, :]
                    nb = cur[comp, z + 2, x0:x0 + width, :]
                    nb = nb + cur[comp, z, x0:x0 + width, :]
                    nb = nb + cur[comp, z + 1, x0 + 1:x0 + 1 + width, :]
                    nb = nb + cur[comp, z + 1, x0 - 1:x0 - 1 + width, :]
                    nb = nb + jnp.where(lane == 0, 0.0, pltpu.roll(mid, 1, 1))
                    nb = nb + jnp.where(lane == ny - 1, 0.0, pltpu.roll(mid, ny - 1, 1))
                    total = total + MU * nb
                sums.append(total)
            c_re = coef[0, z, x0:x0 + width, :]
            c_im = coef[1, z, x0:x0 + width, :]
            new[0, z + 1, x0:x0 + width, :] = c_re * sums[0] - c_im * sums[1]
            new[1, z + 1, x0:x0 + width, :] = c_re * sums[1] + c_im * sums[0]
            return carry

        lax.fori_loop(0, nz, plane, 0, unroll=2)

    last = u0 if SWEEPS % 2 else u1

    def d_copy(ch, j):
        d = across(j)
        t2, s2 = d // slabs, lax.rem(d, slabs)
        return pltpu.make_async_remote_copy(
            last.at[:, pl.ds(1 + s2 * depth, depth), xrow(ch, t2, LOW), :],
            back.at[me, :, :, kept(ch), :],
            s_d, r_d.at[ch], device_id=(t2, s2), device_id_type=MESH)

    def own_d(ch):
        return pltpu.make_async_copy(
            last.at[:, pl.ds(1 + s * depth, depth), xrow(ch, t, LOW), :],
            back.at[me, :, :, kept(ch), :], loc.at[3, 0, ch])

    def others(ch):
        return hat.at[pl.ds(0, devices - 1), :, :, kept(ch), :]

    for c in range(chunks + 1):
        if c < chunks:
            own_b(c).wait()
            wait_bytes(others(c), r_b.at[c])
        for j in range(SWEEPS):
            tile(c, j, xstep if c < chunks else LOW)
        if c > 0:
            for j in order:
                d_copy(c - 1, j).start()
            own_d(c - 1).start()
    shrink = [math.exp(-math.log(ALPHA) * n / steps) / steps for n in range(steps)]

    def f_copy(arr, ch, j):
        t2 = lax.rem(t + j, groups)
        ref = so_ref if arr == 0 else ao_ref
        return pltpu.make_async_remote_copy(
            outs.at[arr, pl.ds(t2 * local, local), :, kept(ch), :],
            ref.at[:, :, xrow(ch, t), :],
            s_f.at[ch, arr, j - 1], r_f.at[ch, arr, j - 1],
            device_id=(t2, s), device_id_type=MESH)

    def own_f(arr, ch):
        ref = so_ref if arr == 0 else ao_ref
        return pltpu.make_async_copy(
            outs.at[arr, pl.ds(t * local, local), :, kept(ch), :],
            ref.at[:, :, xrow(ch, t), :], loc.at[4, arr, ch])

    def backward(ch, c):
        wait_bytes(others(ch), r_d.at[ch])
        own_d(ch).wait()

        def piece(z, c):
            at = kept(ch)

            def load(k):
                return back[k, 0, z, at, :], back[k, 1, z, at, :]

            for n, (re, im) in enumerate(fft_list(load, list(range(steps)), 1)):
                outs[0, n, z, at, :] = re * shrink[n]
                outs[1, steps - 1 - n, z, at, :] = im * shrink[n]
            return c

        lax.fori_loop(0, depth, piece, 0)
        for arr in range(2):
            for j in range(1, groups):
                f_copy(arr, ch, j).start()
            own_f(arr, ch).start()
        return c

    lax.fori_loop(0, chunks, backward, 0)
    def finish(ch, c):
        for j in range(1, groups):
            for arr in range(2):
                a_copy(arr, ch, j).wait_send()
                f_copy(arr, ch, j).wait()
        for arr in range(2):
            own_f(arr, ch).wait()
        return c

    lax.fori_loop(0, chunks, finish, 0)
    most = hat.at[pl.ds(0, devices - 1)]
    wait_bytes(most, s_b)
    wait_bytes(most, s_d)
    wait_bytes(planes_of(slabs // 2 - 1), s_r)
    wait_bytes(planes_of(slabs // 2), s_y)


def fused_body(state_rhs, adjoint_rhs, reaction):
    groups, slabs = lax.axis_size("tm"), lax.axis_size("space")
    local, depth, nx, ny = state_rhs.shape
    dims = (groups, slabs, local, depth, nx, ny)
    steps, devices, nz, xb = groups * local, groups * slabs, depth * slabs, nx // groups
    chunks = xb // 8
    edged = LOW + nx + HIGH
    turn = 2.0 * math.pi * np.arange(steps) / steps
    rate = ALPHA ** (1.0 / steps)
    lam = np.stack((1.0 - rate * np.cos(turn), rate * np.sin(turn)), axis=1).astype(np.float32)
    f32 = jnp.float32
    dma = pltpu.SemaphoreType.DMA
    vmem = pl.BlockSpec(memory_space=pltpu.VMEM)
    shape = jax.ShapeDtypeStruct(state_rhs.shape, f32)
    return pl.pallas_call(
        functools.partial(whole_kernel, dims),
        out_shape=(shape, shape),
        in_specs=[pl.BlockSpec(memory_space=pltpu.SMEM), vmem, vmem, vmem],
        out_specs=(vmem, vmem),
        scratch_shapes=[
            pltpu.VMEM((2, steps, depth, xb, ny), f32),
            pltpu.VMEM((devices, 2, depth, xb, ny), f32),
            pltpu.VMEM((2, nz, edged, ny), f32),
            pltpu.VMEM((nz, nx, ny), f32),
            pltpu.VMEM((2, nz, edged, ny), f32),
            pltpu.VMEM((2, nz + 2, edged, ny), f32),
            pltpu.VMEM((2, nz + 2, edged, ny), f32),
            pltpu.VMEM((devices, 2, depth, xb, ny), f32),
            pltpu.VMEM((2, steps, depth, xb, ny), f32),
            dma((chunks, 2, groups - 1)),
            dma((chunks, 2, groups - 1)),
            dma,
            dma((chunks,)),
            dma,
            dma((chunks,)),
            dma((chunks, 2, groups - 1)),
            dma((chunks, 2, groups - 1)),
            dma,
            dma,
            dma,
            dma,
            dma,
            dma,
            dma((5, 2, chunks)),
        ],
        compiler_params=pltpu.CompilerParams(
            has_side_effects=True, vmem_limit_bytes=58 * 1024 * 1024
        ),
    )(jnp.asarray(lam), state_rhs, adjoint_rhs, reaction)


def solution(mesh):
    in_specs = (P("tm", "space", None, None), P("tm", "space", None, None), P("space", None, None))
    out_specs = (P("tm", "space", None, None), P("tm", "space", None, None))
    groups, slabs = mesh.shape["tm"], mesh.shape["space"]

    def chosen(state_rhs, adjoint_rhs, reaction):
        steps = state_rhs.shape[0] * groups
        fits = steps == groups * slabs and steps & (steps - 1) == 0 and groups % 2 == 0
        fits = fits and slabs % 2 == 0 and slabs > 2 and state_rhs.shape[3] % 128 == 0
        fits = fits and state_rhs.shape[2] % (8 * groups) == 0 and SWEEPS <= LOW <= 8 * groups
        return (fused_body if fits else body)(state_rhs, adjoint_rhs, reaction)

    return jax.shard_map(chosen, mesh=mesh, in_specs=in_specs, out_specs=out_specs, check_vma=False)
```
